16 devices in a mesh: rep: 4 (over y, z, core), dp: 4 (over x).
Axes of the slice: x: 4, y: 2, z: 1, core: 2. Of those that a mesh axis runs over, the one named last changes fastest.
The devices are a block of a 4x4x8 slice.
Arguments:
- x: bfloat16 [16, 4096, 896], P(('rep', 'dp')), parts along dimension 0
- dy: bfloat16 [16, 4096, 896], P(('rep', 'dp')), parts along dimension 0
- w_gate: bfloat16 [2, 896, 2560], P(None, 'dp')
- w_up: bfloat16 [2, 896, 2560], P(None, 'dp')
- w_down: bfloat16 [2, 2560, 896], P(None, 'dp')
Outputs:
- output 1: bfloat16 [16, 4096, 896], P(('rep', 'dp')), parts along dimension 0
- output 2: bfloat16 [8, 896, 2560], P('rep', 'dp'), parts along dimension 0
- output 3: bfloat16 [8, 896, 2560], P('rep', 'dp'), parts along dimension 0
- output 4: bfloat16 [8, 2560, 896], P('rep', 'dp'), parts along dimension 0
There are 4 independent parts. The reference program is written for one: setup_inputs(seed, part) draws one part's arguments, and reference() takes and returns one part's arrays. A program takes and returns all parts, laid end to end along the dimension named above; an argument that names none is the same for every part.
All inputs are finite; a program needn't handle non-finite values.
Results may differ from the reference program's by a relative error of at most 0.018.
Values are sent between devices in bfloat16 or wider.
A program may use at most 768 MiB of HBM per device.

```python
import jax
import jax.numpy as jnp
from jax import lax

SEQUENCES = 4
TOKENS = 4096
D = 896
FF = 2560
LAYERS = 2
NAMES = ("w_gate", "w_up", "w_down")
SHAPES = {"w_gate": (LAYERS, D, FF), "w_up": (LAYERS, D, FF), "w_down": (LAYERS, FF, D)}


def bump(key, n, height):
    away = (jnp.arange(n, dtype=jnp.int32) - jax.random.randint(key, (), 0, n, jnp.int32)) % n
    return jnp.where(away < n // 8, height, 1.0)


def together(key, own, strength):
    shared = jax.random.normal(key, own.shape[1:], jnp.float32)
    return (own + strength * shared) * lax.rsqrt(1 + strength * strength)


def setup_inputs(seed: int = 0, part: int = 0) -> dict:
    kx, kdy, ka, kb, kz, kf, kh, kl, *kw = jax.random.split(jax.random.key(seed), 8 + len(NAMES))
    kx, kdy, ka, kb = (jax.random.fold_in(k, part) for k in (kx, kdy, ka, kb))
    shape = (SEQUENCES, TOKENS, D)
    much_x, much_dy = jax.random.uniform(kz, (2,), jnp.float32, 0.0, 1.0)
    layers = 2.0 ** jax.random.uniform(kl, (LAYERS, 1, 1), jnp.float32, -1.0, 1.0)
    x = together(ka, jax.random.normal(kx, shape, jnp.float32), much_x) * bump(kf, D, 4.0)
    dy = together(kb, jax.random.normal(kdy, shape, jnp.float32), much_dy)
    drawn = {"x": x.astype(jnp.bfloat16), "dy": (dy * (SEQUENCES * TOKENS) ** -0.5).astype(jnp.bfloat16)}
    for key, name in zip(kw, NAMES, strict=True):
        w = jax.random.normal(key, SHAPES[name], jnp.float32) * SHAPES[name][1] ** -0.5
        drawn[name] = (w * {"w_gate": 1.0, "w_up": bump(kh, FF, 4.0), "w_down": layers}[name]).astype(jnp.bfloat16)
    return drawn


def matmul(a, w):
    return jnp.dot(a, w, preferred_element_type=jnp.float32).astype(jnp.bfloat16)


def normed(h):
    wide = h.astype(jnp.float32)
    scale = lax.rsqrt(jnp.mean(wide**2, -1, keepdims=True) + 1e-6)
    return (wide * scale).astype(jnp.bfloat16)


def layer(h, w):
    a = normed(h)
    gate = jnp.dot(a, w["w_gate"], preferred_element_type=jnp.float32)
    up = jnp.dot(a, w["w_up"], preferred_element_type=jnp.float32)
    return h + matmul((jax.nn.silu(gate) * up).astype(jnp.bfloat16), w["w_down"])


def stack(weights, h):
    return lax.scan(lambda h, w: (layer(h, w), None), h, weights)[0]


def reference(x, dy, w_gate, w_up, w_down):
    weights = dict(zip(NAMES, (w_gate, w_up, w_down), strict=True))

    def take(so_far, sequence):
        h, by_y = sequence
        _, back = jax.vjp(stack, weights, h)
        by_weights, by_h = back(by_y)
        return jax.tree.map(lambda total, term: total + term.astype(jnp.float32), so_far, by_weights), by_h

    none_yet = {name: jnp.zeros(w.shape, jnp.float32) for name, w in weights.items()}
    by_weights, by_x = lax.scan(take, none_yet, (x, dy))
    return (by_x, *(by_weights[name].astype(jnp.bfloat16) for name in NAMES))
```

```python
import functools

import jax
import jax.numpy as jnp
from jax import lax
from jax.experimental import pallas as pl
from jax.experimental.pallas import tpu as pltpu
from jax.sharding import PartitionSpec as P

F32, BF16 = jnp.float32, jnp.bfloat16
LANES = 128
VMEM_LIMIT = 62 * 1024 * 1024


def dot(a, b, dims=((1,), (0,))):
    return lax.dot_general(a, b, (dims, ((), ())), preferred_element_type=F32)


def rms_scale(wide):
    return lax.rsqrt(jnp.mean(wide * wide, -1, keepdims=True) + 1e-6)


def normed(h):
    wide = h.astype(F32)
    return (wide * rms_scale(wide)).astype(BF16)


def slot(d, rows, core, part):
    return pl.ds(pl.multiple_of(d * rows + core * part, 16), part)


class Item:
    def __init__(self, ref, own, columns=None):
        self.ref, self.own, self.columns = ref, own, columns

    def half(self, d, core, quarter=None):
        if self.columns is None:
            rows = self.ref.shape[0] // self.own
            part = rows // 2
            if quarter is None:
                return self.ref.at[slot(d, rows, core, part)]
            part //= 2
            return self.ref.at[slot(d, rows, 2 * core + quarter, part)]
        rows = self.ref.shape[1] // self.own
        first, width = self.columns
        if quarter is not None:
            width //= 2
            first += quarter * width
        return self.ref.at[:, slot(d, rows, core, rows // 2), pl.ds(first, width)]


def forward_kernel(dp, n, nt, x_ref, wg_in, wu_in, wd_in, h_ref, a_ref, g_ref, u_ref, wgu_out, wd_out, gu, wd0, kept_a, hidden, send_sem, recv_sem, own_sem, out_sem):
    p, i = pl.program_id(0), pl.program_id(1)
    step = p * nt + i
    tile, part = g_ref.shape[1:]
    rows = pl.ds(pl.multiple_of(i * tile, tile), tile)

    me, rep = lax.axis_index("dp"), lax.axis_index("rep")
    core = lax.rem(rep, 2)
    right, left, far = lax.rem(me + 1, dp), lax.rem(me + dp - 1, dp), lax.rem(me + 2, dp)
    to_right, to_left, to_partner = {"dp": right}, {"dp": left}, {"rep": rep + 1 - 2 * core}

    items = [Item(gu.at[0], dp, (j * part, part)) for j in range(n)]
    items += [Item(wd0, dp)]
    cut = 2 * part
    items += [Item(gu.at[1], dp, (0, cut)), Item(gu.at[1], dp, (cut, n * part - cut))]
    items += [Item(wd_out.at[1], dp)]
    last = len(items) - 1

    def copy(k, s, ref, device, src=None):
        return pltpu.make_async_remote_copy(
            src_ref=ref if src is None else src,
            dst_ref=ref,
            send_sem=send_sem.at[k, s],
            recv_sem=recv_sem.at[k, s],
            device_id=device,
            device_id_type=pl.DeviceIdType.MESH,
        )

    def near(k):
        t = items[k]
        half = t.half(me, core)
        src = None
        if k == last:
            size = half.shape[0]
            src = wd_in.at[1, pl.ds(pl.multiple_of(core * size, 16), size)]
        return [copy(k, 0, half, to_right, src), copy(k, 1, half, to_left, src)]

    def onward(k):
        t = items[k]
        return [
            copy(k, 2, t.half(left, core, 0), to_right),
            copy(k, 3, t.half(right, core, 1), to_left),
        ]

    def across(k, c):
        t = items[k]
        return [
            copy(k, 4, t.half(left, c), to_partner),
            copy(k, 5, t.half(right, c), to_partner),
            copy(k, 6, t.half(far, c, 0), to_partner),
            copy(k, 7, t.half(far, c, 1), to_partner),
        ]

    def send_near(k):
        for c in near(k):
            c.start()

    def send_on(k):
        t = items[k]
        copy(k, 0, t.half(left, core), to_right).wait_recv()
        copy(k, 1, t.half(right, core), to_left).wait_recv()
        for c in onward(k) + across(k, core)[:2]:
            c.start()

    def send_across(k):
        t = items[k]
        copy(k, 2, t.half(far, core, 0), to_right).wait_recv()
        copy(k, 3, t.half(far, core, 1), to_left).wait_recv()
        for c in across(k, core)[2:]:
            c.start()

    def arrive(k):
        for c in across(k, 1 - core):
            c.wait_recv()

    def own(k):
        wide = lambda layer, m, w: pltpu.make_async_copy(w.at[layer], gu.at[layer, m, slot(me, w.shape[1], 0, w.shape[1])], own_sem.at[k])
        down = wd_in.shape[1]
        return [
            lambda: wide(0, 0, wg_in),
            lambda: wide(0, 1, wu_in),
            lambda: pltpu.make_async_copy(wd_in.at[0], wd0.at[slot(me, down, 0, down)], own_sem.at[k]),
            lambda: wide(1, 0, wg_in),
            lambda: wide(1, 1, wu_in),
            lambda: pltpu.make_async_copy(wd_in.at[1], wd_out.at[1, slot(me, down, 0, down)], own_sem.at[k]),
        ][k]()

    def out(k):
        return pltpu.make_async_copy(*[(gu.at[0], wgu_out.at[0]), (wd0, wd_out.at[0]), (gu.at[1], wgu_out.at[1])][k], out_sem.at[k])

    @pl.when(step == 0)
    def _():
        barrier = pltpu.get_barrier_semaphore()
        for k in range(6):
            own(k).start()
        for device in (to_right, to_left, to_partner):
            pl.semaphore_signal(barrier, inc=1, device_id=device, device_id_type=pl.DeviceIdType.MESH)
        pl.semaphore_wait(barrier, 3)
        own(0).wait()
        own(1).wait()
        send_near(0)
        send_on(0)
        send_near(1)
        send_across(0)
        for k in range(2, 5):
            own(k).wait()
        arrive(0)

    def at(phase, tile_index, *actions):
        @pl.when(step == phase * nt + tile_index * nt // 8)
        def _():
            for f, k in actions:
                f(k)

    for k in range(1, n):
        s = 3 + 7 * (k - 1)
        at(0, s, (send_on, k), (send_near, k + 1))
        at(0, s + 3, (send_across, k))
        at(k, 0, (arrive, k))
    at(n - 1, 6, (send_on, n), (send_near, n + 1))
    at(n, 0, (send_across, n), (arrive, n), (lambda k: (out(0).start(), out(1).start()), 0))
    at(n, 4, (send_on, n + 1), (send_near, n + 2))
    at(n, 6, (send_across, n + 1))
    at(n + 1, 0, (arrive, n + 1))
    at(n + 2, 1, (send_on, n + 2), (send_near, n + 3))
    at(n + 2, 7, (send_across, n + 2))
    at(n + 3, 0, (arrive, n + 2), (lambda k: out(2).start(), 0))
    at(n + 4, 4, (send_on, n + 3))
    at(n + 5, 4, (send_across, n + 3))

    @pl.when(p == 0)
    def _():
        a = normed(x_ref[...])
        kept_a[rows] = a
        a_ref[0] = a

    def gate_up(layer, j):
        a = kept_a[rows]
        at = pl.ds(pl.multiple_of(j * part, part), part)
        g, u = dot(a, gu[layer, 0, :, at]), dot(a, gu[layer, 1, :, at])
        g_ref[0], u_ref[0] = g, u
        return g, u, at

    @pl.when(p < n)
    def _():
        g, u, at = gate_up(0, p)
        hidden[rows, at] = (g * jax.nn.sigmoid(g) * u).astype(BF16)

    @pl.when(p == n)
    def _():
        h = x_ref[...] + dot(hidden[rows, :], wd0[...]).astype(BF16)
        h_ref[...] = h
        a = normed(h)
        kept_a[rows] = a
        a_ref[0] = a

    @pl.when(p > n)
    def _():
        gate_up(1, p - n - 1)

    @pl.when(step == (2 * n + 1) * nt - 1)
    def _():
        arrive(last)
        for k in range(len(items)):
            for c in near(k) + onward(k) + across(k, core):
                c.wait_send()
        own(5).wait()
        for k in range(3):
            out(k).wait()


def forward(dp, n, x, wg, wu, wd, tile=512):
    tokens, d = x.shape
    ff = wg.shape[2]
    part, nt = ff // n, tokens // tile
    end = nt - 1

    def x_at(p, i):
        return jnp.where((p == 0) | (p == n), i, end), 0

    def h_at(p, i):
        return jnp.where(p < n, 0, jnp.where(p == n, i, end)), 0

    def a_at(p, i):
        return jnp.where(p < n, 0, 1), jnp.where((p == 0) | (p == n), i, end), 0

    def g_at(p, i):
        second = p > n
        return jnp.where(second, 1, 0), jnp.where(p == n, end, i), jnp.where(second, p - n - 1, jnp.minimum(p, n - 1))

    kept = pl.BlockSpec((1, tile, part), g_at)
    anywhere = pl.BlockSpec(memory_space=pl.ANY)
    wide = jax.ShapeDtypeStruct((2, tokens, ff), F32)
    return pl.pallas_call(
        functools.partial(forward_kernel, dp, n, nt),
        name="forward",
        grid=(2 * n + 1, nt),
        in_specs=[pl.BlockSpec((tile, d), x_at)] + [anywhere] * 3,
        out_specs=[pl.BlockSpec((tile, d), h_at), pl.BlockSpec((1, tile, d), a_at), kept, kept, anywhere, anywhere],
        out_shape=[
            jax.ShapeDtypeStruct((tokens, d), BF16),
            jax.ShapeDtypeStruct((2, tokens, d), BF16),
            wide,
            wide,
            jax.ShapeDtypeStruct((2, 2, d, ff), BF16),
            jax.ShapeDtypeStruct((2, ff, d), BF16),
        ],
        scratch_shapes=[
            pltpu.VMEM((2, 2, d, ff), BF16),
            pltpu.VMEM((ff, d), BF16),
            pltpu.VMEM((tokens, d), BF16),
            pltpu.VMEM((tokens, ff), BF16),
            pltpu.SemaphoreType.DMA((n + 4, 8)),
            pltpu.SemaphoreType.DMA((n + 4, 8)),
            pltpu.SemaphoreType.DMA((6,)),
            pltpu.SemaphoreType.DMA((3,)),
        ],
        compiler_params=pltpu.CompilerParams(
            dimension_semantics=("arbitrary", "arbitrary"), vmem_limit_bytes=67043328, collective_id=0, has_side_effects=True
        ),
        cost_estimate=pl.CostEstimate(flops=10 * tokens * d * ff, transcendentals=tokens * ff, bytes_accessed=16 * tokens * ff),
    )(x, wg, wu, wd)


def backward_kernel(dp, first, last, *refs):
    refs = list(refs)
    take = lambda k: [refs.pop(0) for _ in range(k)]
    a_ref, dy_ref = take(2)
    wg = jnp.concatenate([r[...] for r in take(dp)], axis=1)
    wu = jnp.concatenate([r[...] for r in take(dp)], axis=1)
    wd = jnp.concatenate([r[...] for r in take(dp)], axis=0)
    g = jnp.concatenate([r[...] for r in take(dp)], axis=1)
    u = jnp.concatenate([r[...] for r in take(dp)], axis=1)
    (da_in,) = (None,) if first else take(1)
    (h_ref,) = take(1) if last else (None,)
    da_ref, out_ref = take(2)
    acc_g, acc_u, acc_d = take(3)
    step, steps = pl.program_id(0), pl.num_programs(0)

    a, dy = a_ref[...], dy_ref[...]
    dh = dot(dy, wd, ((1,), (1,))).astype(BF16).astype(F32)
    s = jax.nn.sigmoid(g)
    silu = g * s
    hidden = (silu * u).astype(BF16)
    du = (dh * silu).astype(BF16)
    dg = (dh * u * (s * (1.0 + g * (1.0 - s)))).astype(BF16)
    da = dot(dg, wg, ((1,), (1,))) + dot(du, wu, ((1,), (1,)))
    if da_in is not None:
        da = da + da_in[...]
    if last:
        wide = h_ref[...].astype(F32)
        scale = rms_scale(wide)
        c = da.astype(BF16).astype(F32)
        back = scale * c - wide * (scale * scale * scale * jnp.mean(c * wide, -1, keepdims=True))
        da_ref[...] = dy + back.astype(BF16)
    else:
        da_ref[...] = da

    @pl.when(step == 0)
    def _():
        acc_g[...] = jnp.zeros_like(acc_g)
        acc_u[...] = jnp.zeros_like(acc_u)
        acc_d[...] = jnp.zeros_like(acc_d)

    acc_g[...] += dot(a, dg, ((0,), (0,)))
    acc_u[...] += dot(a, du, ((0,), (0,)))
    acc_d[...] += dot(dy, hidden, ((0,), (0,)))

    @pl.when(step == steps - 1)
    def _():
        d, part = acc_g.shape
        rows, run = d // dp, part // dp
        for owner in range(dp):
            for k, acc in enumerate((acc_g, acc_u)):
                for q in range(dp):
                    at = (k * dp + q) * rows
                    out_ref[owner, at : at + rows, :] = acc[owner * rows : (owner + 1) * rows, q * run : (q + 1) * run].astype(BF16)
            base = 2 * dp * rows
            for q in range(d // LANES):
                block = acc_d[q * LANES : (q + 1) * LANES, owner * run : (owner + 1) * run]
                out_ref[owner, base + q * run : base + (q + 1) * run, :] = block.T.astype(BF16)


def backward(dp, n, j, layer, a, dy, wgu, wd, g, u, da, h, tile=512):
    tokens, d = dy.shape
    ff = wd.shape[1]
    part = ff // n
    run = part // dp
    first, last = da is None, h is not None
    rows = pl.BlockSpec((tile, d), lambda i: (i, 0))
    of_layer = pl.BlockSpec((None, tile, d), lambda i: (layer, i, 0))
    one = pl.Buffered(1)
    columns = [pl.BlockSpec((None, None, d, run), lambda i, m=m, q=q: (layer, m, 0, q * n + j), pipeline_mode=one) for m in range(2) for q in range(dp)]
    lines = [pl.BlockSpec((None, run, d), lambda i, q=q: (layer, q * n + j, 0), pipeline_mode=one) for q in range(dp)]
    wide = [pl.BlockSpec((None, tile, run), lambda i, q=q: (layer, i, q * n + j)) for q in range(dp)]
    args = [a, dy] + [wgu] * 2 * dp + [wd] * dp + [g] * dp + [u] * dp
    specs = [of_layer, rows] + columns + lines + wide * 2
    if not first:
        args.append(da)
        specs.append(rows)
    if last:
        args.append(h)
        specs.append(rows)
    size = 3 * d
    return pl.pallas_call(
        functools.partial(backward_kernel, dp, first, last),
        name="backward",
        grid=(tokens // tile,),
        in_specs=specs,
        out_specs=[rows, pl.BlockSpec((dp, size, LANES), lambda i: (0, 0, 0), pipeline_mode=one)],
        out_shape=[jax.ShapeDtypeStruct((tokens, d), BF16 if last else F32), jax.ShapeDtypeStruct((dp, size, LANES), BF16)],
        scratch_shapes=[pltpu.VMEM((d, part), F32)] * 3,
        compiler_params=pltpu.CompilerParams(dimension_semantics=("arbitrary",), vmem_limit_bytes=VMEM_LIMIT),
        cost_estimate=pl.CostEstimate(
            flops=12 * tokens * d * part, transcendentals=tokens * part, bytes_accessed=8 * tokens * (part + 2 * d)
        ),
    )(*args)


def layer_back(dp, n, layer, a, dy, wgu, wd, g, u, h):
    da, sums = None, []
    for j in range(n):
        da, terms = backward(dp, n, j, layer, a, dy, wgu, wd, g, u, da, h if j == n - 1 else None)
        sums.append(lax.psum_scatter(terms, "dp", scatter_dimension=0, tiled=True)[0])
    return da, sums


def assemble_kernel(dp, n, layers, *refs):
    sums, outs = refs[: layers * n], refs[layers * n :]
    for layer in range(layers):
        for j in range(n):
            t = sums[layer * n + j]
            for m in range(2):
                rows = outs[m].shape[1]
                for q in range(dp):
                    at = (m * dp + q) * rows
                    outs[m][layer, :, (q * n + j) * LANES : (q * n + j + 1) * LANES] = t[at : at + rows, :]
            d = outs[2].shape[2]
            run = outs[2].shape[1] // n
            for q in range(d // LANES):
                at = 2 * d + q * run
                outs[2][layer, j * run : (j + 1) * run, q * LANES : (q + 1) * LANES] = t[at : at + run, :]


def assembled(dp, n, shapes, sums):
    layers = shapes[0][0]
    inside = pl.BlockSpec(memory_space=pltpu.VMEM)
    return pl.pallas_call(
        functools.partial(assemble_kernel, dp, n, layers),
        name="assemble",
        in_specs=[inside] * len(sums),
        out_specs=[inside] * 3,
        out_shape=[jax.ShapeDtypeStruct(s, BF16) for s in shapes],
        compiler_params=pltpu.CompilerParams(vmem_limit_bytes=VMEM_LIMIT),
    )(*sums)


def solution(mesh):
    dp = mesh.shape["dp"]

    def step(x, dy, wg, wu, wd):
        x, dy = x[0], dy[0]
        n = wg.shape[2] // (dp * LANES)
        h1, a, g, u, wgu, wdown = forward(dp, n, x, wg, wu, wd)
        dh1, sums1 = layer_back(dp, n, 1, a, dy, wgu, wdown, g, u, h1)
        dx, sums0 = layer_back(dp, n, 0, a, dh1, wgu, wdown, g, u, x)
        return (dx[None], *assembled(dp, n, [w.shape for w in (wg, wu, wd)], sums0 + sums1))

    tokens, w = P(("rep", "dp"), None, None), P(None, "dp", None)
    return jax.shard_map(
        step,
        mesh=mesh,
        in_specs=(tokens, tokens, w, w, w),
        out_specs=(tokens, *[P("rep", "dp", None)] * 3),
        check_vma=False,
    )
```

```python
import functools

import jax
import jax.numpy as jnp
from jax import lax
from jax.experimental import pallas as pl
from jax.experimental.pallas import tpu as pltpu
from jax.sharding import PartitionSpec as P

F32, BF16 = jnp.float32, jnp.bfloat16
LANES = 128
VMEM_LIMIT = 62 * 1024 * 1024


def dot(a, b, dims=((1,), (0,))):
    return lax.dot_general(a, b, (dims, ((), ())), preferred_element_type=F32)


def rms_scale(wide):
    return lax.rsqrt(jnp.mean(wide * wide, -1, keepdims=True) + 1e-6)


def normed(h):
    wide = h.astype(F32)
    return (wide * rms_scale(wide)).astype(BF16)


def slot(d, rows, core, part):
    return pl.ds(pl.multiple_of(d * rows + core * part, 16), part)


class Item:
    def __init__(self, ref, own, columns=None):
        self.ref, self.own, self.columns = ref, own, columns

    def half(self, d, core, quarter=None):
        if self.columns is None:
            rows = self.ref.shape[0] // self.own
            part = rows // 2
            if quarter is None:
                return self.ref.at[slot(d, rows, core, part)]
            part //= 2
            return self.ref.at[slot(d, rows, 2 * core + quarter, part)]
        rows = self.ref.shape[1] // self.own
        first, width = self.columns
        if quarter is not None:
            width //= 2
            first += quarter * width
        return self.ref.at[:, slot(d, rows, core, rows // 2), pl.ds(first, width)]


def forward_kernel(dp, n, nt, x_ref, wg_in, wu_in, wd_in, h_ref, a_ref, g_ref, u_ref, wgu_out, wd_out, gu, wd0, kept_a, hidden, send_sem, recv_sem, own_sem, out_sem):
    p, i = pl.program_id(0), pl.program_id(1)
    step = p * nt + i
    tile, part = g_ref.shape[1:]
    rows = pl.ds(pl.multiple_of(i * tile, tile), tile)

    me, rep = lax.axis_index("dp"), lax.axis_index("rep")
    core = lax.rem(rep, 2)
    right, left, far = lax.rem(me + 1, dp), lax.rem(me + dp - 1, dp), lax.rem(me + 2, dp)
    to_right, to_left, to_partner = {"dp": right}, {"dp": left}, {"rep": rep + 1 - 2 * core}

    items = [Item(gu.at[0], dp, (j * part, part)) for j in range(n)]
    items += [Item(wd0, dp)]
    cut = 2 * part
    items += [Item(gu.at[1], dp, (0, cut)), Item(gu.at[1], dp, (cut, n * part - cut))]
    items += [Item(wd_out.at[1], dp)]
    last = len(items) - 1

    def copy(k, s, ref, device, src=None):
        return pltpu.make_async_remote_copy(
            src_ref=ref if src is None else src,
            dst_ref=ref,
            send_sem=send_sem.at[k, s],
            recv_sem=recv_sem.at[k, s],
            device_id=device,
            device_id_type=pl.DeviceIdType.MESH,
        )

    def near(k):
        t = items[k]
        half = t.half(me, core)
        src = None
        if k == last:
            size = half.shape[0]
            src = wd_in.at[1, pl.ds(pl.multiple_of(core * size, 16), size)]
        return [copy(k, 0, half, to_right, src), copy(k, 1, half, to_left, src)]

    def onward(k):
        t = items[k]
        return [
            copy(k, 2, t.half(left, core, 0), to_right),
            copy(k, 3, t.half(right, core, 1), to_left),
        ]

    def across(k, c):
        t = items[k]
        return [
            copy(k, 4, t.half(left, c), to_partner),
            copy(k, 5, t.half(right, c), to_partner),
            copy(k, 6, t.half(far, c, 0), to_partner),
            copy(k, 7, t.half(far, c, 1), to_partner),
        ]

    def send_near(k):
        for c in near(k):
            c.start()

    def send_on(k):
        t = items[k]
        copy(k, 0, t.half(left, core), to_right).wait_recv()
        copy(k, 1, t.half(right, core), to_left).wait_recv()
        for c in onward(k) + across(k, core)[:2]:
            c.start()

    def send_across(k):
        t = items[k]
        copy(k, 2, t.half(far, core, 0), to_right).wait_recv()
        copy(k, 3, t.half(far, core, 1), to_left).wait_recv()
        for c in across(k, core)[2:]:
            c.start()

    def arrive(k):
        for c in across(k, 1 - core):
            c.wait_recv()

    def own(k):
        wide = lambda layer, m, w: pltpu.make_async_copy(w.at[layer], gu.at[layer, m, slot(me, w.shape[1], 0, w.shape[1])], own_sem.at[k])
        down = wd_in.shape[1]
        return [
            lambda: wide(0, 0, wg_in),
            lambda: wide(0, 1, wu_in),
            lambda: pltpu.make_async_copy(wd_in.at[0], wd0.at[slot(me, down, 0, down)], own_sem.at[k]),
            lambda: wide(1, 0, wg_in),
            lambda: wide(1, 1, wu_in),
            lambda: pltpu.make_async_copy(wd_in.at[1], wd_out.at[1, slot(me, down, 0, down)], own_sem.at[k]),
        ][k]()

    def out(k):
        return pltpu.make_async_copy(*[(gu.at[0], wgu_out.at[0]), (wd0, wd_out.at[0]), (gu.at[1], wgu_out.at[1])][k], out_sem.at[k])

    @pl.when(step == 0)
    def _():
        barrier = pltpu.get_barrier_semaphore()
        for k in range(6):
            own(k).start()
        for device in (to_right, to_left, to_partner):
            pl.semaphore_signal(barrier, inc=1, device_id=device, device_id_type=pl.DeviceIdType.MESH)
        pl.semaphore_wait(barrier, 3)
        own(0).wait()
        own(1).wait()
        send_near(0)
        send_on(0)
        send_near(1)
        send_across(0)
        for k in range(2, 5):
            own(k).wait()
        arrive(0)

    def at(phase, tile_index, *actions):
        @pl.when(step == phase * nt + tile_index * nt // 8)
        def _():
            for f, k in actions:
                f(k)

    at(0, 3, (send_on, 1), (send_near, 2), (send_near, 3))
    at(0, 6, (send_across, 1))
    for k, step_on, step_across in ((2, 9, 14), (3, 13, 20), (4, 18, 30)):
        at(0, step_on, (send_on, k), (send_near, k + 2))
        at(0, step_across, (send_across, k))
    for k in range(1, n):
        at(k, 0, (arrive, k))
    at(0, 29, (send_on, n), (send_near, n + 2))
    at(0, 38, (send_on, n + 1), (send_near, n + 3))
    at(n, 0, (send_across, n), (arrive, n), (lambda k: (out(0).start(), out(1).start()), 0))
    at(n, 5, (send_on, n + 2))
    at(n, 6, (send_across, n + 1))
    at(n + 1, 0, (arrive, n + 1))
    at(n + 1, 2, (send_on, n + 3))
    at(n + 2, 1, (send_across, n + 2))
    at(n + 2, 6, (send_across, n + 3))
    at(n + 3, 0, (arrive, n + 2), (lambda k: out(2).start(), 0))

    @pl.when(p == 0)
    def _():
        a = normed(x_ref[...])
        kept_a[rows] = a
        a_ref[0] = a

    def gate_up(layer, j):
        a = kept_a[rows]
        at = pl.ds(pl.multiple_of(j * part, part), part)
        g, u = dot(a, gu[layer, 0, :, at]), dot(a, gu[layer, 1, :, at])
        g_ref[0], u_ref[0] = g, u
        return g, u, at

    @pl.when(p < n)
    def _():
        g, u, at = gate_up(0, p)
        hidden[rows, at] = (g * jax.nn.sigmoid(g) * u).astype(BF16)

    @pl.when(p == n)
    def _():
        h = x_ref[...] + dot(hidden[rows, :], wd0[...]).astype(BF16)
        h_ref[...] = h
        a = normed(h)
        kept_a[rows] = a
        a_ref[0] = a

    @pl.when(p > n)
    def _():
        gate_up(1, p - n - 1)

    @pl.when(step == (2 * n + 1) * nt - 1)
    def _():
        arrive(last)
        for k in range(len(items)):
            for c in near(k) + onward(k) + across(k, core):
                c.wait_send()
        own(5).wait()
        for k in range(3):
            out(k).wait()


def forward(dp, n, x, wg, wu, wd, tile=512):
    tokens, d = x.shape
    ff = wg.shape[2]
    part, nt = ff // n, tokens // tile
    end = nt - 1

    def x_at(p, i):
        return jnp.where((p == 0) | (p == n), i, end), 0

    def h_at(p, i):
        return jnp.where(p < n, 0, jnp.where(p == n, i, end)), 0

    def a_at(p, i):
        return jnp.where(p < n, 0, 1), jnp.where((p == 0) | (p == n), i, end), 0

    def g_at(p, i):
        second = p > n
        return jnp.where(second, 1, 0), jnp.where(p == n, end, i), jnp.where(second, p - n - 1, jnp.minimum(p, n - 1))

    kept = pl.BlockSpec((1, tile, part), g_at)
    anywhere = pl.BlockSpec(memory_space=pl.ANY)
    wide = jax.ShapeDtypeStruct((2, tokens, ff), F32)
    return pl.pallas_call(
        functools.partial(forward_kernel, dp, n, nt),
        name="forward",
        grid=(2 * n + 1, nt),
        in_specs=[pl.BlockSpec((tile, d), x_at)] + [anywhere] * 3,
        out_specs=[pl.BlockSpec((tile, d), h_at), pl.BlockSpec((1, tile, d), a_at), kept, kept, anywhere, anywhere],
        out_shape=[
            jax.ShapeDtypeStruct((tokens, d), BF16),
            jax.ShapeDtypeStruct((2, tokens, d), BF16),
            wide,
            wide,
            jax.ShapeDtypeStruct((2, 2, d, ff), BF16),
            jax.ShapeDtypeStruct((2, ff, d), BF16),
        ],
        scratch_shapes=[
            pltpu.VMEM((2, 2, d, ff), BF16),
            pltpu.VMEM((ff, d), BF16),
            pltpu.VMEM((tokens, d), BF16),
            pltpu.VMEM((tokens, ff), BF16),
            pltpu.SemaphoreType.DMA((n + 4, 8)),
            pltpu.SemaphoreType.DMA((n + 4, 8)),
            pltpu.SemaphoreType.DMA((6,)),
            pltpu.SemaphoreType.DMA((3,)),
        ],
        compiler_params=pltpu.CompilerParams(
            dimension_semantics=("arbitrary", "arbitrary"), vmem_limit_bytes=67043328, collective_id=0, has_side_effects=True
        ),
        cost_estimate=pl.CostEstimate(flops=10 * tokens * d * ff, transcendentals=tokens * ff, bytes_accessed=16 * tokens * ff),
    )(x, wg, wu, wd)


def backward_kernel(dp, first, last, after, *refs):
    refs = list(refs)
    take = lambda k: [refs.pop(0) for _ in range(k)]
    a_ref, dy_ref = take(2)
    wg = jnp.concatenate([r[...] for r in take(dp)], axis=1)
    wu = jnp.concatenate([r[...] for r in take(dp)], axis=1)
    wd = jnp.concatenate([r[...] for r in take(dp)], axis=0)
    g = jnp.concatenate([r[...] for r in take(dp)], axis=1)
    u = jnp.concatenate([r[...] for r in take(dp)], axis=1)
    (da_in,) = (None,) if first else take(1)
    (h_ref,) = take(1) if last else (None,)
    take(1 if after else 0)
    da_ref, out_ref = take(2)
    acc_g, acc_u, acc_d = take(3)
    step, steps = pl.program_id(0), pl.num_programs(0)

    a, dy = a_ref[...], dy_ref[...]
    s = jax.nn.sigmoid(g)
    silu = g * s
    hidden = (silu * u).astype(BF16)
    slope = u * (s * (1.0 + g * (1.0 - s)))
    dh = dot(dy, wd, ((1,), (1,))).astype(BF16).astype(F32)
    du = (dh * silu).astype(BF16)
    dg = (dh * slope).astype(BF16)
    da = dot(jnp.concatenate([dg, du], axis=1), jnp.concatenate([wg, wu], axis=1), ((1,), (1,)))
    if da_in is not None:
        da = da + da_in[...]
    if last:
        wide = h_ref[...].astype(F32)
        scale = rms_scale(wide)
        c = da.astype(BF16).astype(F32)
        back = scale * c - wide * (scale * scale * scale * jnp.mean(c * wide, -1, keepdims=True))
        da_ref[...] = dy + back.astype(BF16)
    else:
        da_ref[...] = da

    @pl.when(step == 0)
    def _():
        acc_g[...] = jnp.zeros_like(acc_g)
        acc_u[...] = jnp.zeros_like(acc_u)
        acc_d[...] = jnp.zeros_like(acc_d)

    acc_g[...] += dot(a, dg, ((0,), (0,)))
    acc_u[...] += dot(a, du, ((0,), (0,)))
    acc_d[...] += dot(dy, hidden, ((0,), (0,)))

    @pl.when(step == steps - 1)
    def _():
        d, part = acc_g.shape
        rows, run = d // dp, part // dp
        for owner in range(dp):
            for k, acc in enumerate((acc_g, acc_u)):
                for q in range(dp):
                    at = (k * dp + q) * rows
                    out_ref[owner, at : at + rows, :] = acc[owner * rows : (owner + 1) * rows, q * run : (q + 1) * run].astype(BF16)
            base = 2 * dp * rows
            for q in range(d // LANES):
                block = acc_d[q * LANES : (q + 1) * LANES, owner * run : (owner + 1) * run]
                out_ref[owner, base + q * run : base + (q + 1) * run, :] = block.T.astype(BF16)


def backward(dp, n, j, layer, a, dy, wgu, wd, g, u, da, h, done, tile=512):
    tokens, d = dy.shape
    ff = wd.shape[1]
    part = ff // n
    run = part // dp
    first, last = da is None, h is not None
    rows = pl.BlockSpec((tile, d), lambda i: (i, 0))
    of_layer = pl.BlockSpec((None, tile, d), lambda i: (layer, i, 0))
    one = pl.Buffered(1)
    columns = [pl.BlockSpec((None, None, d, run), lambda i, m=m, q=q: (layer, m, 0, q * n + j), pipeline_mode=one) for m in range(2) for q in range(dp)]
    lines = [pl.BlockSpec((None, run, d), lambda i, q=q: (layer, q * n + j, 0), pipeline_mode=one) for q in range(dp)]
    wide = [pl.BlockSpec((None, tile, run), lambda i, q=q: (layer, i, q * n + j)) for q in range(dp)]
    args = [a, dy] + [wgu] * 2 * dp + [wd] * dp + [g] * dp + [u] * dp
    specs = [of_layer, rows] + columns + lines + wide * 2
    if not first:
        args.append(da)
        specs.append(rows)
    if last:
        args.append(h)
        specs.append(rows)
    if done is not None:
        args.append(done)
        specs.append(pl.BlockSpec(memory_space=pl.ANY))
    size = 3 * d
    return pl.pallas_call(
        functools.partial(backward_kernel, dp, first, last, done is not None),
        name="backward",
        grid=(tokens // tile,),
        in_specs=specs,
        out_specs=[rows, pl.BlockSpec((dp, size, LANES), lambda i: (0, 0, 0), pipeline_mode=one)],
        out_shape=[jax.ShapeDtypeStruct((tokens, d), BF16 if last else F32), jax.ShapeDtypeStruct((dp, size, LANES), BF16)],
        scratch_shapes=[pltpu.VMEM((d, part), F32)] * 3,
        compiler_params=pltpu.CompilerParams(dimension_semantics=("arbitrary",), vmem_limit_bytes=VMEM_LIMIT),
        cost_estimate=pl.CostEstimate(
            flops=12 * tokens * d * part, transcendentals=tokens * part, bytes_accessed=8 * tokens * (part + 2 * d)
        ),
    )(*args)


def norm_kernel(da_ref, h_ref, dy_ref, done_ref, dx_ref):
    wide = h_ref[...].astype(F32)
    scale = rms_scale(wide)
    c = da_ref[...].astype(BF16).astype(F32)
    back = scale * c - wide * (scale * scale * scale * jnp.mean(c * wide, -1, keepdims=True))
    dx_ref[...] = dy_ref[...] + back.astype(BF16)


def norm_back(da, h, dy, done, tile=512):
    tokens, d = dy.shape
    rows = pl.BlockSpec((tile, d), lambda i: (i, 0))
    return pl.pallas_call(
        norm_kernel,
        name="norm_back",
        grid=(tokens // tile,),
        in_specs=[rows, rows, rows, pl.BlockSpec(memory_space=pl.ANY)],
        out_specs=rows,
        out_shape=jax.ShapeDtypeStruct((tokens, d), BF16),
        compiler_params=pltpu.CompilerParams(dimension_semantics=("arbitrary",)),
        cost_estimate=pl.CostEstimate(flops=20 * tokens * d, transcendentals=tokens, bytes_accessed=10 * tokens * d),
    )(da, h, dy, done)


def layer_back(dp, n, layer, a, dy, wgu, wd, g, u, h, apart, before):
    da, sums = None, list(before)
    for j in range(n):
        done = sums[-2] if len(sums) > 1 else None
        da, terms = backward(dp, n, j, layer, a, dy, wgu, wd, g, u, da, h if j == n - 1 and not apart else None, done)
        sums.append(lax.psum_scatter(terms, "dp", scatter_dimension=0, tiled=True)[0])
    if apart:
        da = norm_back(da, h, dy, sums[-2])
    return da, sums[-n:]


def assemble_kernel(dp, n, *refs):
    sums, outs = refs[:n], refs[-3:]
    for j in range(n):
        t = sums[j]
        for m in range(2):
            rows = outs[m].shape[0]
            for q in range(dp):
                at = (m * dp + q) * rows
                outs[m][:, (q * n + j) * LANES : (q * n + j + 1) * LANES] = t[at : at + rows, :]
        d = outs[2].shape[1]
        run = outs[2].shape[0] // n
        for q in range(d // LANES):
            at = 2 * d + q * run
            outs[2][j * run : (j + 1) * run, q * LANES : (q + 1) * LANES] = t[at : at + run, :]


def assembled(dp, n, shapes, layer, sums, others):
    inside = pl.BlockSpec(memory_space=pltpu.VMEM)
    return pl.pallas_call(
        functools.partial(assemble_kernel, dp, n),
        name="assemble",
        grid=(1,),
        in_specs=[inside] * n + [pl.BlockSpec(memory_space=pl.ANY)] * len(others),
        out_specs=[pl.BlockSpec((None, *s[1:]), lambda i: (layer, 0, 0)) for s in shapes],
        out_shape=[jax.ShapeDtypeStruct(s, BF16) for s in shapes],
        input_output_aliases={n + k: k for k in range(len(others))},
        compiler_params=pltpu.CompilerParams(vmem_limit_bytes=VMEM_LIMIT),
    )(*sums, *others)


def solution(mesh):
    dp = mesh.shape["dp"]

    def step(x, dy, wg, wu, wd):
        x, dy = x[0], dy[0]
        n = wg.shape[2] // (dp * LANES)
        h1, a, g, u, wgu, wdown = forward(dp, n, x, wg, wu, wd)
        dh1, sums1 = layer_back(dp, n, 1, a, dy, wgu, wdown, g, u, h1, False, [])
        dx, sums0 = layer_back(dp, n, 0, a, dh1, wgu, wdown, g, u, x, True, sums1)
        shapes = [w.shape for w in (wg, wu, wd)]
        grads = assembled(dp, n, shapes, 1, sums1, [])
        return (dx[None], *assembled(dp, n, shapes, 0, sums0, grads))

    tokens, w = P(("rep", "dp"), None, None), P(None, "dp", None)
    return jax.shard_map(
        step,
        mesh=mesh,
        in_specs=(tokens, tokens, w, w, w),
        out_specs=(tokens, *[P("rep", "dp", None)] * 3),
        check_vma=False,
    )
```
